128 devices in a mesh: gx: 4 (over x), gy: 8 (over y, core), gz: 4 (over z).
Axes of the slice: x: 4, y: 4, z: 4, core: 2. Of those that a mesh axis runs over, the one named last changes fastest.
Arguments:
- labels: int32 [128, 512, 512], P('gx', 'gy', 'gz'), may hold values from 0 to 7
- conductivity: float32 [7, 8], replicated, may hold values from -0.08 to 2, as said below
- right_side: float32 [128, 512, 512], P('gx', 'gy', 'gz'), may hold values from -18 to 18
Outputs:
- solution: float32 [128, 512, 512], P('gx', 'gy', 'gz')
The draws below stay inside these ranges and needn't reach their ends.
Inputs may be any that keep to these rules, and one draw needn't show every extreme that they name: `conductivity`: rows 0 to 2 are positive, rows 3 to 5 have magnitude at most 0.08, row 6 is at least 0.5.
All inputs are finite; a program needn't handle non-finite values.
Results may differ from the reference program's by a relative error of at most 0.0001.
Values sent between devices are 32-bit elements; how exact they have to be, the bound alone decides.
A program may use at most 128 MiB of HBM per device.

```python
import math
import jax
import jax.numpy as jnp
from jax import lax

ITERS = 3
LABELS = 8
NX = 128
NY = 512
NZ = 512


def draw_conductivity(key, part):
    key_diag = jax.random.fold_in(key, 11)
    key_off = jax.random.fold_in(key, 12)
    key_mass = jax.random.fold_in(key, 13)
    diagonal = jnp.exp(jax.random.uniform(key_diag, (3, LABELS), jnp.float32, math.log(0.5), math.log(2.0)))
    offdiag = jax.random.uniform(key_off, (3, LABELS), jnp.float32, -0.08, 0.08)
    mass = jnp.exp(jax.random.uniform(key_mass, (1, LABELS), jnp.float32, math.log(0.5), math.log(1.0)))
    return jnp.concatenate([diagonal, offdiag, mass], axis=0).astype(jnp.float32)


def draw_right_side(key, part):
    key_base = jax.random.fold_in(key, 21)
    key_scale = jax.random.fold_in(key, 22)
    column = jnp.exp(jax.random.uniform(key_scale, (NX, NY, 1), jnp.float32, math.log(0.3), math.log(3.0)))
    ramp = 0.5 + jnp.arange(NY, dtype=jnp.float32)[None, :, None] / NY
    base = jnp.clip(jax.random.normal(key_base, (NX, NY, NZ), jnp.float32), -3.6, 3.6)
    return (base * column * ramp + 1.0).astype(jnp.float32)


def place_ends(array, stream_key, low, top_value):
    index_at = [jax.random.randint(jax.random.fold_in(stream_key, axis), (), 0, length) for axis, length in enumerate(array.shape)]
    widest = array.shape.index(max(array.shape))
    neighbour = index_at[:widest] + [(index_at[widest] + 1) % array.shape[widest]] + index_at[widest + 1:]
    return array.at[tuple(index_at)].set(low).at[tuple(neighbour)].set(top_value)


def setup_inputs(seed: int = 0) -> dict:
    arg_keys = jax.random.split(jax.random.key(seed), 4)
    labels = place_ends(jax.random.randint(arg_keys[0], (NX, NY, NZ), 0, LABELS), jax.random.fold_in(arg_keys[0], 1), 0, LABELS - 1).astype(jnp.int32)
    conductivity = draw_conductivity(jax.random.fold_in(arg_keys[3], 71), 0)
    right_side = draw_right_side(jax.random.fold_in(arg_keys[3], 71), 0)
    return {"labels": labels, "conductivity": conductivity, "right_side": right_side}


def neighbour_value(arr, shift_x, shift_y, shift_z, cell_grid):
    size_x, size_y, size_z = cell_grid
    return arr[..., 1 + shift_x:1 + shift_x + size_x, 1 + shift_y:1 + shift_y + size_y, 1 + shift_z:1 + shift_z + size_z]


def stencil_apply(padded_value, padded_sigma, self_coefficient):
    cell_grid = self_coefficient.shape
    value_entry = neighbour_value(padded_value, 0, 0, 0, cell_grid)
    total_flux = self_coefficient * value_entry
    for axis in range(3):
        for sign in (-1, 1):
            stencil_offset = [0, 0, 0]
            stencil_offset[axis] = sign
            face_flux = 0.5 * (neighbour_value(padded_sigma[axis], 0, 0, 0, cell_grid) + neighbour_value(padded_sigma[axis], stencil_offset[0], stencil_offset[1], stencil_offset[2], cell_grid))
            total_flux = total_flux + face_flux * (value_entry - neighbour_value(padded_value, stencil_offset[0], stencil_offset[1], stencil_offset[2], cell_grid))
    for first, second, comp in ((0, 1, 3), (0, 2, 4), (1, 2, 5)):
        for sign_a in (-1, 1):
            for sign_b in (-1, 1):
                stencil_offset = [0, 0, 0]
                stencil_offset[first] = sign_a
                stencil_offset[second] = sign_b
                cross_term = (0.25 * sign_a * sign_b) * (neighbour_value(padded_sigma[comp], 0, 0, 0, cell_grid) + neighbour_value(padded_sigma[comp], stencil_offset[0], stencil_offset[1], stencil_offset[2], cell_grid))
                total_flux = total_flux - cross_term * neighbour_value(padded_value, stencil_offset[0], stencil_offset[1], stencil_offset[2], cell_grid)
    return total_flux


def diagonal_of(padded_sigma, self_coefficient):
    cell_grid = self_coefficient.shape
    total_flux = self_coefficient
    for axis in range(3):
        for sign in (-1, 1):
            stencil_offset = [0, 0, 0]
            stencil_offset[axis] = sign
            total_flux = total_flux + 0.5 * (neighbour_value(padded_sigma[axis], 0, 0, 0, cell_grid) + neighbour_value(padded_sigma[axis], stencil_offset[0], stencil_offset[1], stencil_offset[2], cell_grid))
    return total_flux


def reference(labels, conductivity, right_side):
    extended = jnp.concatenate([jnp.zeros((7, 1), conductivity.dtype), conductivity], axis=1)
    label_pad = jnp.pad(labels.astype(jnp.int32) + 1, 1)
    planes = jnp.arange(labels.shape[0], dtype=jnp.int32)

    def slab_table(index):
        part = lax.dynamic_slice_in_dim(label_pad, index, 3, 0)
        table = jnp.take(extended, part, axis=1)
        return table[:6], table[6, 1:2, 1:-1, 1:-1]

    def diag_plane(index):
        padded_sigma, self_coefficient = slab_table(index)
        return diagonal_of(padded_sigma, self_coefficient)[0]

    diag = lax.map(diag_plane, planes)

    def operate(field):
        field_pad = jnp.pad(field, 1)

        def one_plane(index):
            padded_sigma, self_coefficient = slab_table(index)
            part = lax.dynamic_slice_in_dim(field_pad, index, 3, 0)
            return stencil_apply(part, padded_sigma, self_coefficient)[0]

        return lax.map(one_plane, planes)

    solution = jnp.zeros_like(right_side)
    residual = right_side
    precond = residual / diag
    direction = precond
    gamma = jnp.sum(residual * precond)
    for step in range(ITERS):
        image = operate(direction)
        alpha = gamma / jnp.sum(direction * image)
        solution = solution + alpha * direction
        residual = residual - alpha * image
        precond = residual / diag
        fresh = jnp.sum(residual * precond)
        direction = precond + (fresh / gamma) * direction
        gamma = fresh
    return solution
```

```python
import functools

import jax
import jax.numpy as jnp
from jax import lax
from jax.experimental import pallas as pl
from jax.experimental.pallas import tpu as pltpu
from jax.sharding import PartitionSpec as P

MESH = pl.DeviceIdType.MESH
W = 4
LAYERS = 12
OUTSIDE = 8
DIRS = tuple((a, b) for a in (-1, 0, 1) for b in (-1, 0, 1) if (a, b) != (0, 0))
UNROLL = 2


def row_groups(lo, hi):
    starts = list(range(lo, hi - 7, 8))
    if starts[-1] + 8 < hi:
        starts.append(hi - 8)
    return starts


def group_spans(lo, hi, first, last):
    spans, done = [], first
    for start in row_groups(lo, hi):
        low, high = max(done, start), min(last, start + 8)
        done = max(done, high)
        spans.append((start, low - start, max(high, low) - start))
    return spans


def kernel(sizes, cond, lab_hbm, b_hbm, out, *scr):
    (gxn, gyn, gzn, X, Y) = sizes
    PX, PY = X + 2 * W, Y + 2 * W
    (e_lab, e_b, e_sig, e_inv, e_v, e_tmp, k_lab, k_b, k_sig, k_inv, k_v, k_tmp, kint, kt, ar, arslot,
     load_sem, s1, r1, s2, r2, sa, ra) = scr
    gx, gy, gz = lax.axis_index("gx"), lax.axis_index("gy"), lax.axis_index("gz")

    load_lab = pltpu.make_async_copy(lab_hbm, e_lab.at[pl.ds(W, X), pl.ds(W, Y), :], load_sem.at[0])
    load_b = pltpu.make_async_copy(b_hbm, e_b.at[pl.ds(W, X), pl.ds(W, Y), :], load_sem.at[1])
    load_lab.start()
    load_b.start()

    def exists(dx, dy):
        ok = None
        for pos, d, n in ((gx, dx, gxn), (gy, dy, gyn)):
            if d:
                here = (pos + d >= 0) & (pos + d < n)
                ok = here if ok is None else ok & here
        return ok

    barrier = pltpu.get_barrier_semaphore()
    for axis, pos, n in (("gy", gy, gyn), ("gx", gx, gxn), ("gz", gz, gzn)):
        for d in range(1, n):
            pl.semaphore_signal(barrier, inc=1, device_id={axis: lax.rem(pos + d, n)}, device_id_type=MESH)
    peers = gyn - 1 + gxn - 1 + gzn - 1
    for dx, dy in DIRS:
        if dx and dy:
            ok = exists(dx, dy)

            @pl.when(ok)
            def _():
                pl.semaphore_signal(barrier, inc=1, device_id={"gx": gx + dx, "gy": gy + dy}, device_id_type=MESH)

            peers = peers + ok.astype(jnp.int32)
    pl.semaphore_wait(barrier, peers)

    def region(d, n, width, arriving):
        if d == 0:
            return pl.ds(W, n)
        if arriving:
            return pl.ds(W + n, width) if d < 0 else pl.ds(W - width, width)
        return pl.ds(W, width) if d < 0 else pl.ds(W + n - width, width)

    def phase1(i, field):
        dx, dy = DIRS[i]
        ref, width = ((e_lab, W), (e_b, W - 1))[field]
        src = ref.at[region(dx, X, width, False), region(dy, Y, width, False), :]
        dst = ref.at[region(dx, X, width, True), region(dy, Y, width, True), :]
        target = {}
        if dx:
            target["gx"] = jnp.clip(gx + dx, 0, gxn - 1)
        if dy:
            target["gy"] = jnp.clip(gy + dy, 0, gyn - 1)
        return pltpu.make_async_remote_copy(
            src_ref=src, dst_ref=dst, send_sem=s1.at[i, field], recv_sem=r1.at[i, field],
            device_id=target, device_id_type=MESH)

    for field, load in ((0, load_lab), (1, load_b)):
        load.wait()
        for i, (dx, dy) in enumerate(DIRS):
            @pl.when(exists(dx, dy))
            def _():
                phase1(i, field).start()

    def fill_e(xs, nx, ys, ny):
        def body(m, c):
            e_lab[xs + m, pl.ds(ys, ny), :] = jnp.full((ny, 128), OUTSIDE, jnp.int32)
            e_b[xs + m, pl.ds(ys, ny), :] = jnp.zeros((ny, 128), jnp.float32)
            return c
        lax.fori_loop(0, nx, body, 0)

    @pl.when(gx == 0)
    def _():
        fill_e(0, W, 0, PY)

    @pl.when(gx == gxn - 1)
    def _():
        fill_e(W + X, W, 0, PY)

    @pl.when(gy == 0)
    def _():
        fill_e(0, PX, 0, W)

    @pl.when(gy == gyn - 1)
    def _():
        fill_e(0, PX, W + Y, W)

    def fill_k(side, layer):
        rows = pl.ds((side * LAYERS + layer) * PX, W * PX)
        k_lab[rows, :] = jnp.full((W * PX, 128), OUTSIDE, jnp.int32)
        k_b[rows, :] = jnp.zeros((W * PX, 128), jnp.float32)

    @pl.when(gz == 0)
    def _():
        fill_k(0, 0)

    @pl.when(gz == gzn - 1)
    def _():
        fill_k(1, 2 * W)

    for field in (0, 1):
        for i, (dx, dy) in enumerate(DIRS):
            @pl.when(exists(-dx, -dy))
            def _():
                phase1(i, field).wait_recv()

    def extract(m, c):
        for src, dst in ((e_lab, k_lab), (e_b, k_b)):
            plane = jnp.concatenate([src[m], jnp.zeros((128 - PY, 128), src.dtype)], axis=0)
            turned = plane.T
            dst[pl.ds(4 * PX + m, 8, stride=PX), :] = turned[0:8]
            dst[pl.ds(LAYERS * PX + m, 8, stride=PX), :] = turned[120:128]
        return c

    lax.fori_loop(0, PX, extract, 0, unroll=2)

    def phase2(up, field):
        ref, width = ((k_lab, W), (k_b, W - 1))[field]
        if up:
            src, dst = LAYERS + 8 - width, W - width
        else:
            src, dst = W, LAYERS + 8
        target = {"gz": jnp.clip(gz + (1 if up else -1), 0, gzn - 1)}
        return pltpu.make_async_remote_copy(
            src_ref=ref.at[pl.ds(src * PX, width * PX), :], dst_ref=ref.at[pl.ds(dst * PX, width * PX), :],
            send_sem=s2.at[up, field], recv_sem=r2.at[up, field], device_id=target, device_id_type=MESH)

    has = (gz > 0, gz < gzn - 1)
    for field in (0, 1):
        for up in (0, 1):
            @pl.when(has[up])
            def _():
                phase2(up, field).start()

    sub = lax.broadcasted_iota(jnp.int32, (8, 128), 0)
    lane = lax.broadcasted_iota(jnp.int32, (8, 128), 1)
    factor = (0.5, 0.5, 0.5, 0.25, 0.25, 0.25, 1.0)
    tables = []
    for c in range(7):
        tab = jnp.zeros((8, 128), jnp.float32)
        for label in range(8):
            tab = jnp.where(sub == label, cond[c, label], tab)
        tables.append(tab * factor[c])

    def lookup(lab):
        inside = lab < OUTSIDE
        index = jnp.bitwise_and(lab, 7)
        return [
            jnp.where(inside, jnp.take_along_axis(t, index, axis=0, mode="promise_in_bounds"), 0.0) for t in tables
        ], inside

    class Box:
        pass

    E, K = Box(), Box()
    E.ld = lambda ref, m, s: ref[m, pl.ds(s, 8), :]
    E.lab, E.b, E.inv = e_lab, e_b, e_inv
    E.sig = [e_sig.at[c] for c in range(7)]
    E.v = [e_v.at[k] for k in range(3)]
    E.tmp = [e_tmp.at[k] for k in range(5)]
    E.names = dict(m=0, s=1, l=2, ms=3, ml=4, sl=5)
    K.ld = lambda ref, m, s: ref[pl.ds(m * PX + s, 8), :]
    K.lab, K.b, K.inv = k_lab, k_b, k_inv
    K.sig = [k_sig.at[c] for c in range(7)]
    K.v = [k_v.at[k] for k in range(3)]
    K.tmp = [k_tmp.at[k] for k in range(5)]
    K.names = dict(m=2, s=0, l=1, ms=4, ml=5, sl=3)

    def e_st(ref, m, s, val):
        ref[m, pl.ds(s, 8), :] = val

    def k_st(ref, m, s, val):
        ref[pl.ds(m * PX + s, 8), :] = val

    E.st, K.st = e_st, k_st
    zero = jnp.zeros((8, 128), jnp.float32)
    left = lambda t: pltpu.roll(t, 127, 1)
    right = lambda t: pltpu.roll(t, 1, 1)

    def e_loop(halo, body, init):
        lo, count = W - halo, X + 2 * halo
        step = UNROLL

        def run(t, c):
            for u in range(step):
                c = body(lo + t * step + u, c)
            return c
        return lax.fori_loop(0, count // step, run, init)

    def k_loop(halo, body, init):
        def run(t, c):
            c = body(4 - halo + t, c)
            return body(LAYERS + 7 - halo + t, c)
        return lax.fori_loop(0, 2 * halo + 1, run, init)

    E.loop, K.loop = e_loop, k_loop
    E.span, K.span = Y, X
    E.inner = lambda m: (m >= W) & (m < W + X)
    K.inner = lambda m: (m == 4) | (m == LAYERS + 7)
    E.edge = (lane == 0) | (lane == 127)

    def insert(k, m, s, val):
        turned = pltpu.roll(kt[k, pl.ds(s, 8), :], lax.rem(255 - 2 * m, 128), 1)
        return jnp.where(E.edge, turned, val)

    E.insert = insert
    K.insert = lambda k, m, s, val: val

    def spans(box, halo):
        return group_spans(W - halo, W + box.span + halo, W, W + box.span)

    def masked(val, span, inner):
        start, low, high = span
        if low >= high:
            return None
        if (low, high) != (0, 8):
            val = jnp.where((sub >= low) & (sub < high), val, 0.0)
        return jnp.where(inner, val, 0.0)

    def stage_sigma(box, halo):
        def body(m, c):
            for s, _, _ in spans(box, W):
                sig, inside = lookup(box.ld(box.lab, m, s))
                for k in range(7):
                    box.st(box.sig[k], m, s, sig[k])
            return c
        box.loop(halo, body, 0)

    def stage_diag(box):
        nm = box.names
        sm, ss, sl = box.sig[nm["m"]], box.sig[nm["s"]], box.sig[nm["l"]]

        def body(m, acc):
            inner = box.inner(m)
            for span in spans(box, 3):
                s = span[0]
                cl = box.ld(sl, m, s)
                cm, cs = box.ld(sm, m, s), box.ld(ss, m, s)
                total = box.ld(box.sig[6], m, s) + 2.0 * (cl + cm + cs)
                total = total + box.ld(sm, m - 1, s) + box.ld(sm, m + 1, s)
                total = total + box.ld(ss, m, s - 1) + box.ld(ss, m, s + 1)
                total = total + left(cl) + right(cl)
                inv = jnp.where(box.ld(box.lab, m, s) < OUTSIDE, 1.0 / total, 0.0)
                b = box.ld(box.b, m, s)
                v0 = box.insert(0, m, s, b * inv)
                box.st(box.inv, m, s, inv)
                box.st(box.v[0], m, s, v0)
                part = masked(b * v0, span, inner)
                if part is not None:
                    acc = acc + part
            return acc
        return box.loop(3, body, zero)

    def stage_apply(box, k):
        nm = box.names
        v = box.v[k]
        sig = {name: box.sig[i] for name, i in nm.items()}
        t_ms, t_sl, t_s, t_d, t_z = box.tmp
        halo = 3 - k

        def first(m, c):
            for s, _, _ in spans(box, halo):
                val = box.ld(v, m, s)
                up, down = left(val), right(val)
                box.st(t_ms, m, s, box.ld(sig["ms"], m, s) * val)
                box.st(t_sl, m, s, box.ld(sig["sl"], m, s) * val)
                box.st(t_s, m, s, box.ld(sig["s"], m, s) * val)
                box.st(t_d, m, s, up - down)
                box.st(t_z, m, s, box.ld(sig["l"], m, s) * (up + down))
            return c
        box.loop(halo, first, 0)

        def second(m, accs):
            acc0, acc1 = accs
            inner = box.inner(m)
            for span in spans(box, halo - 1):
                s = span[0]
                ld = lambda ref, dm, ds: box.ld(ref, m + dm, s + ds)
                val = ld(v, 0, 0)
                hi, lo = ld(v, 1, 0), ld(v, -1, 0)
                g = ld(sig["m"], 0, 0) * (hi + lo)
                g = g + ld(sig["m"], 1, 0) * hi + ld(sig["m"], -1, 0) * lo
                cross = (ld(v, 1, 1) - ld(v, 1, -1)) - (ld(v, -1, 1) - ld(v, -1, -1))
                g = g + ld(sig["ms"], 0, 0) * cross
                g = g + ((ld(t_ms, 1, 1) - ld(t_ms, 1, -1)) - (ld(t_ms, -1, 1) - ld(t_ms, -1, -1)))
                g = g + ld(sig["s"], 0, 0) * (ld(v, 0, 1) + ld(v, 0, -1)) + (ld(t_s, 0, 1) + ld(t_s, 0, -1))
                g = g + ld(t_z, 0, 0)
                g = g + ld(sig["ml"], 0, 0) * (ld(t_d, 1, 0) - ld(t_d, -1, 0))
                g = g + ld(sig["sl"], 0, 0) * (ld(t_d, 0, 1) - ld(t_d, 0, -1))
                q = (ld(sig["ml"], 1, 0) * hi - ld(sig["ml"], -1, 0) * lo) + (ld(t_sl, 0, 1) - ld(t_sl, 0, -1))
                p = ld(sig["l"], 0, 0) * val
                g = g + left(p + q) + right(p - q)
                part = masked(val * g, span, inner)
                if part is not None:
                    acc0 = acc0 + part
                if k < 2:
                    nxt = box.insert(k + 1, m, s, g * ld(box.inv, 0, 0))
                    box.st(box.v[k + 1], m, s, nxt)
                    part = masked(nxt * g, span, inner)
                    if part is not None:
                        acc1 = acc1 + part
            return acc0, acc1
        return box.loop(halo - 1, second, (zero, zero))

    def stages(box):
        sums = [stage_diag(box)]
        for k in range(3):
            sums += stage_apply(box, k)
        return sums[:6]

    for field in (0, 1):
        for up in (0, 1):
            @pl.when(has[1 - up])
            def _():
                phase2(up, field).wait_recv()

    stage_sigma(K, 4)
    k_sums = stages(K)
    for k in range(3):
        kint[pl.ds(0, PX, stride=2), :] = k_v[k, pl.ds((LAYERS + 7) * PX, PX), :]
        kint[pl.ds(1, PX, stride=2), :] = k_v[k, pl.ds(4 * PX, PX), :]
        kt[k] = kint[...].T
    stage_sigma(E, 4)
    e_sums = stages(E)

    wide = lane[0:1]
    tile = zero
    for k in range(6):
        from_k = jnp.where((wide >= W) & (wide < W + Y), jnp.sum(k_sums[k], axis=0, keepdims=True), 0.0)
        from_e = jnp.where((wide > 0) & (wide < 127), jnp.sum(e_sums[k], axis=0, keepdims=True), 0.0)
        tile = jnp.where(sub == k, from_k + from_e, tile)

    stage = 0
    slot = 0
    for axis, pos, n in (("gy", gy, gyn), ("gx", gx, gxn), ("gz", gz, gzn)):
        ar[stage] = tile
        copies = []
        for d in range(1, n):
            copy = pltpu.make_async_remote_copy(
                src_ref=ar.at[stage], dst_ref=arslot.at[slot], send_sem=sa.at[slot], recv_sem=ra.at[slot],
                device_id={axis: lax.rem(pos + d, n)}, device_id_type=MESH)
            copy.start()
            copies.append((copy, slot))
            slot += 1
        for copy, where in copies:
            copy.wait_recv()
        for copy, where in copies:
            tile = tile + arslot[where]
        for copy, where in copies:
            copy.wait_send()
        stage += 1

    total = jnp.sum(tile, axis=1, keepdims=True)
    n = [jnp.broadcast_to(total[k:k + 1], (8, 128)) for k in range(6)]
    a = [n[k] - n[k + 1] for k in range(5)]
    safe = lambda num, den: jnp.where(den > 0, num / jnp.where(den > 0, den, 1.0), 0.0)
    l1, l2 = safe(a[1], a[0]), safe(a[2], a[0])
    d1 = a[2] - l1 * a[1]
    l21 = safe(a[3] - l1 * a[2], d1)
    d2 = a[4] - l2 * a[2] - l21 * (a[3] - l1 * a[2])
    y1 = n[1] - l1 * n[0]
    y2 = n[2] - l2 * n[0] - l21 * y1
    c2 = safe(y2, d2)
    c1 = safe(y1, d1) - l21 * c2
    c0 = safe(n[0], a[0]) - l1 * c1 - l2 * c2

    def finish(m, c):
        for s in range(0, Y, 8):
            out[m, pl.ds(s, 8), :] = (c0 * e_v[0, m + W, pl.ds(s + W, 8), :] + c1 * e_v[1, m + W, pl.ds(s + W, 8), :]
                                      + c2 * e_v[2, m + W, pl.ds(s + W, 8), :])
        return c

    lax.fori_loop(0, X, finish, 0, unroll=2)

    for field in (0, 1):
        for i, (dx, dy) in enumerate(DIRS):
            @pl.when(exists(dx, dy))
            def _():
                phase1(i, field).wait_send()
        for up in (0, 1):
            @pl.when(has[up])
            def _():
                phase2(up, field).wait_send()


def local(labels, conductivity, right_side, sizes):
    gxn, gyn, gzn = sizes
    X, Y, Z = labels.shape
    assert Z == 128 and Y % 8 == 0
    PX, PY = X + 2 * W, Y + 2 * W
    krows = 2 * LAYERS * PX
    f32 = jnp.float32
    slots = gxn + gyn + gzn - 3
    dma = pltpu.SemaphoreType.DMA
    return pl.pallas_call(
        functools.partial(kernel, (gxn, gyn, gzn, X, Y)),
        out_shape=jax.ShapeDtypeStruct((X, Y, Z), f32),
        in_specs=[
            pl.BlockSpec(memory_space=pltpu.SMEM),
            pl.BlockSpec(memory_space=pl.ANY),
            pl.BlockSpec(memory_space=pl.ANY),
        ],
        out_specs=pl.BlockSpec(memory_space=pltpu.VMEM),
        scratch_shapes=[
            pltpu.VMEM((PX, PY, 128), jnp.int32),
            pltpu.VMEM((PX, PY, 128), f32),
            pltpu.VMEM((7, PX, PY, 128), f32),
            pltpu.VMEM((PX, PY, 128), f32),
            pltpu.VMEM((3, PX, PY, 128), f32),
            pltpu.VMEM((5, PX, PY, 128), f32),
            pltpu.VMEM((krows, 128), jnp.int32),
            pltpu.VMEM((krows, 128), f32),
            pltpu.VMEM((7, krows, 128), f32),
            pltpu.VMEM((krows, 128), f32),
            pltpu.VMEM((3, krows, 128), f32),
            pltpu.VMEM((5, krows, 128), f32),
            pltpu.VMEM((128, 128), f32),
            pltpu.VMEM((3, 128, 128), f32),
            pltpu.VMEM((3, 8, 128), f32),
            pltpu.VMEM((slots, 8, 128), f32),
            dma((2,)), dma((8, 2)), dma((8, 2)), dma((2, 2)), dma((2, 2)), dma((slots,)), dma((slots,)),
        ],
        compiler_params=pltpu.CompilerParams(
            collective_id=0, has_side_effects=True, vmem_limit_bytes=62 * 1024 * 1024),
    )(conductivity, labels, right_side)


def solution(mesh):
    sizes = (mesh.shape["gx"], mesh.shape["gy"], mesh.shape["gz"])
    spec = P("gx", "gy", "gz")
    return jax.shard_map(
        functools.partial(local, sizes=sizes), mesh=mesh, in_specs=(spec, P(), spec), out_specs=spec, check_vma=False)
```

```python
import functools
import itertools
import math

import jax
import jax.numpy as jnp
from jax import lax
from jax.experimental import pallas as pl
from jax.experimental.pallas import tpu as pltpu
from jax.sharding import PartitionSpec as P

MESH = pl.DeviceIdType.MESH
W = 4
LAYERS = 12
OUTSIDE = 8
DIRS = tuple((a, b) for a in (-1, 0, 1) for b in (-1, 0, 1) if (a, b) != (0, 0))
STAGES = (("gx", "gy"), ("gz",))


def row_groups(lo, hi):
    starts = list(range(lo, hi - 7, 8))
    if starts[-1] + 8 < hi:
        starts.append(hi - 8)
    return starts


def group_spans(lo, hi, first, last):
    spans, done = [], first
    for start in row_groups(lo, hi):
        low, high = max(done, start), min(last, start + 8)
        done = max(done, high)
        spans.append((start, low - start, max(high, low) - start))
    return spans


def kernel(sizes, cond, lab_hbm, b_hbm, out, *scr):
    (gxn, gyn, gzn, X, Y) = sizes
    PX, PY = X + 2 * W, Y + 2 * W
    (e_lab, e_b, e_arr, k_lab, k_b, k_arr, kint, kt, ar, arslot,
     load_sem, s1, r1, s2, r2, sa, ra, greet) = scr
    gx, gy, gz = lax.axis_index("gx"), lax.axis_index("gy"), lax.axis_index("gz")

    load_lab = pltpu.make_async_copy(lab_hbm, e_lab.at[pl.ds(W, X), pl.ds(W, Y), :], load_sem.at[0])
    load_b = pltpu.make_async_copy(b_hbm, e_b.at[pl.ds(W, X), pl.ds(W, Y), :], load_sem.at[1])
    load_lab.start()
    load_b.start()

    def exists(dx, dy):
        ok = None
        for pos, d, n in ((gx, dx, gxn), (gy, dy, gyn)):
            if d:
                here = (pos + d >= 0) & (pos + d < n)
                ok = here if ok is None else ok & here
        return ok

    ring = {"gx": (gx, gxn), "gy": (gy, gyn), "gz": (gz, gzn)}

    def peers_of(axes):
        return [d for d in itertools.product(*[range(ring[a][1]) for a in axes]) if any(d)]

    def peer(axes, d):
        return {a: lax.rem(ring[a][0] + k, ring[a][1]) for a, k in zip(axes, d) if k}

    barrier = pltpu.get_barrier_semaphore()
    count = 0
    for axis in ("gy", "gx", "gz"):
        for d in peers_of((axis,)):
            pl.semaphore_signal(barrier, inc=1, device_id=peer((axis,), d), device_id_type=MESH)
            count = count + 1
    for dx, dy in DIRS:
        if dx and dy:
            ok = exists(dx, dy)

            @pl.when(ok)
            def _():
                pl.semaphore_signal(barrier, inc=1, device_id={"gx": gx + dx, "gy": gy + dy}, device_id_type=MESH)

            count = count + ok.astype(jnp.int32)
    pl.semaphore_wait(barrier, count)

    def pass_on(i, axis):
        for d in peers_of((axis,)):
            pl.semaphore_signal(greet.at[i], inc=1, device_id=peer((axis,), d), device_id_type=MESH)

    pass_on(0, "gx")

    def region(d, n, width, arriving):
        if d == 0:
            return pl.ds(W, n)
        if arriving:
            return pl.ds(W + n, width) if d < 0 else pl.ds(W - width, width)
        return pl.ds(W, width) if d < 0 else pl.ds(W + n - width, width)

    def phase1(i, field):
        dx, dy = DIRS[i]
        ref, width = ((e_lab, W), (e_b, W - 1))[field]
        src = ref.at[region(dx, X, width, False), region(dy, Y, width, False), :]
        dst = ref.at[region(dx, X, width, True), region(dy, Y, width, True), :]
        target = {}
        if dx:
            target["gx"] = jnp.clip(gx + dx, 0, gxn - 1)
        if dy:
            target["gy"] = jnp.clip(gy + dy, 0, gyn - 1)
        return pltpu.make_async_remote_copy(
            src_ref=src, dst_ref=dst, send_sem=s1.at[i, field], recv_sem=r1.at[i, field],
            device_id=target, device_id_type=MESH)

    for field, load in ((0, load_lab), (1, load_b)):
        load.wait()
        for i, (dx, dy) in enumerate(DIRS):
            @pl.when(exists(dx, dy))
            def _():
                phase1(i, field).start()

    def fill_e(xs, nx, ys, ny):
        def body(m, c):
            e_lab[xs + m, pl.ds(ys, ny), :] = jnp.full((ny, 128), OUTSIDE, jnp.int32)
            e_b[xs + m, pl.ds(ys, ny), :] = jnp.zeros((ny, 128), jnp.float32)
            return c
        lax.fori_loop(0, nx, body, 0)

    @pl.when(gx == 0)
    def _():
        fill_e(0, W, 0, PY)

    @pl.when(gx == gxn - 1)
    def _():
        fill_e(W + X, W, 0, PY)

    @pl.when(gy == 0)
    def _():
        fill_e(0, PX, 0, W)

    @pl.when(gy == gyn - 1)
    def _():
        fill_e(0, PX, W + Y, W)

    def fill_k(side, layer):
        rows = pl.ds((side * LAYERS + layer) * PX, W * PX)
        k_lab[rows, :] = jnp.full((W * PX, 128), OUTSIDE, jnp.int32)
        k_b[rows, :] = jnp.zeros((W * PX, 128), jnp.float32)

    @pl.when(gz == 0)
    def _():
        fill_k(0, 0)

    @pl.when(gz == gzn - 1)
    def _():
        fill_k(1, 2 * W)

    def arrive(pick):
        for field in (0, 1):
            for i, (dx, dy) in enumerate(DIRS):
                if pick(dx, dy):
                    @pl.when(exists(-dx, -dy))
                    def _():
                        phase1(i, field).wait_recv()

    def phase2(up, field):
        ref, width = ((k_lab, W), (k_b, W - 1))[field]
        if up:
            src, dst = LAYERS + 8 - width, W - width
        else:
            src, dst = W, LAYERS + 8
        target = {"gz": jnp.clip(gz + (1 if up else -1), 0, gzn - 1)}
        return pltpu.make_async_remote_copy(
            src_ref=ref.at[pl.ds(src * PX, width * PX), :], dst_ref=ref.at[pl.ds(dst * PX, width * PX), :],
            send_sem=s2.at[up, field], recv_sem=r2.at[up, field], device_id=target, device_id_type=MESH)

    has = (gz > 0, gz < gzn - 1)

    sub = lax.broadcasted_iota(jnp.int32, (8, 128), 0)
    lane = lax.broadcasted_iota(jnp.int32, (8, 128), 1)
    factor = (0.5, 0.5, 0.5, 0.25, 0.25, 0.25, 1.0)
    tables = []
    for c in range(7):
        tab = jnp.zeros((8, 128), jnp.float32)
        for label in range(8):
            tab = jnp.where(sub == label, cond[c, label], tab)
        tables.append(tab * factor[c])

    def lookup(lab):
        inside = lab < OUTSIDE
        index = jnp.bitwise_and(lab, 7)
        return [
            jnp.where(inside, jnp.take_along_axis(t, index, axis=0, mode="promise_in_bounds"), 0.0) for t in tables
        ], inside

    class Box:
        pass

    E, K = Box(), Box()
    E.at = lambda m, s: (m, pl.ds(s, 8), slice(None))
    K.at = lambda m, s: (pl.ds(m * PX + s, 8), slice(None))
    for box, lab, rhs, arrays in ((E, e_lab, e_b, e_arr), (K, k_lab, k_b, k_arr)):
        box.lab, box.b = lab, rhs
        box.sig = [arrays.at[c] for c in range(7)]
        box.fm, box.fs, box.fl, box.fr, box.cpp, box.cpm, box.inv = [arrays.at[7 + c] for c in range(7)]
        box.v = [arrays.at[14 + c] for c in range(3)]
        ping, pong = (arrays.at[17], arrays.at[18]), (arrays.at[19], arrays.at[20])
        box.t = [ping, pong, ping]
    E.names, K.names = (0, 1, 2, 3, 4, 5), (2, 0, 1, 4, 5, 3)
    E.span, K.span = Y, X
    E.inner = lambda m: (m >= W) & (m < W + X)
    zero = jnp.zeros((8, 128), jnp.float32)
    left = lambda t: pltpu.roll(t, 127, 1)
    right = lambda t: pltpu.roll(t, 1, 1)

    class Cells:
        def __init__(self, box, m):
            self.box, self.m, self.seen = box, m, {}

        def __call__(self, ref, dm, s):
            key = (id(ref), dm, s)
            if key not in self.seen:
                self.seen[key] = ref[self.box.at(self.m + dm, s)]
            return self.seen[key]

    def run(loop, body, init):
        base, stride, trips, _ = loop
        return lax.fori_loop(0, trips, lambda t, c: body(base + t * stride, c), init)

    def spans(box, halo):
        return group_spans(W - halo, W + box.span + halo, W, W + box.span)

    def clip(val, span):
        _, low, high = span
        if low >= high:
            return None
        if (low, high) != (0, 8):
            val = jnp.where((sub >= low) & (sub < high), val, 0.0)
        return val

    def add(total, val):
        return val if total is None else total if val is None else total + val

    def gather(box, m, acc, parts, inner):
        for u, part in enumerate(parts):
            if part is not None and (inner is None or inner == "ask" or u in inner):
                acc = acc + (jnp.where(box.inner(m + u), part, 0.0) if inner == "ask" else part)
        return acc

    def sigma(box, loop, starts):
        def body(m, c):
            for s in starts:
                for u in range(loop[3]):
                    sig, _ = lookup(box.lab[box.at(m + u, s)])
                    for k in range(7):
                        box.sig[k][box.at(m + u, s)] = sig[k]
            return c
        run(loop, body, 0)

    def spread(box, m, s, v, fl, fr):
        up, down = left(v), right(v)
        box.t[0][0][box.at(m, s)] = up - down
        box.t[0][1][box.at(m, s)] = fl * up + fr * down

    def diagonal(box, loop, inner, acc):
        sm, ss, sl, ms = [box.sig[box.names[i]] for i in range(4)]

        def body(m, acc):
            ld = Cells(box, m)
            parts = [None] * loop[3]
            for span in spans(box, 3):
                s = span[0]
                for u in range(loop[3]):
                    at = box.at(m + u, s)
                    cm, cs, cl, cx = ld(sm, u, s), ld(ss, u, s), ld(sl, u, s), ld(ms, u, s)
                    fm, fs = cm + ld(sm, u + 1, s), cs + ld(ss, u, s + 1)
                    fl, fr = cl + left(cl), cl + right(cl)
                    total = (ld(box.sig[6], u, s) + fm + (cm + ld(sm, u - 1, s))) + (fs + (cs + ld(ss, u, s - 1)))
                    total = total + (fl + fr)
                    inv = jnp.where(ld(box.lab, u, s) < OUTSIDE, 1.0 / total, 0.0)
                    b = ld(box.b, u, s)
                    v0 = b * inv
                    box.fm[at], box.fs[at], box.fl[at], box.fr[at] = fm, fs, fl, fr
                    box.cpp[at] = cx + ld(ms, u + 1, s + 1)
                    box.cpm[at] = -(cx + ld(ms, u + 1, s - 1))
                    box.inv[at] = inv
                    box.v[0][at] = v0
                    spread(box, m + u, s, v0, fl, fr)
                    parts[u] = add(parts[u], clip(b * v0, span))
            return gather(box, m, acc, parts, inner)
        return run(loop, body, acc)

    def apply(box, k, loop, inner, accs):
        v, ml, sl = box.v[k], box.sig[box.names[4]], box.sig[box.names[5]]

        def body(m, accs):
            ld = Cells(box, m)
            nxt_td = {}
            parts0, parts1 = [None] * loop[3], [None] * loop[3]
            for span in spans(box, 2 - k):
                s = span[0]
                for u in range(loop[3]):
                    at = box.at(m + u, s)
                    val, hi, lo = ld(v, u, s), ld(v, u + 1, s), ld(v, u - 1, s)
                    up, down = ld(v, u, s + 1), ld(v, u, s - 1)
                    a1 = ld(box.fm, u, s) * hi + ld(box.fm, u - 1, s) * lo
                    a2 = ld(box.fs, u, s) * up + ld(box.fs, u, s - 1) * down
                    a3 = ld(box.cpp, u, s) * ld(v, u + 1, s + 1) + ld(box.cpp, u - 1, s - 1) * ld(v, u - 1, s - 1)
                    a4 = ld(box.cpm, u, s) * ld(v, u + 1, s - 1) + ld(box.cpm, u - 1, s + 1) * ld(v, u - 1, s + 1)
                    q = (ld(ml, u + 1, s) * hi - ld(ml, u - 1, s) * lo) + (
                        ld(sl, u, s + 1) * up - ld(sl, u, s - 1) * down)
                    a5 = ld(ml, u, s) * (ld(tin, u + 1, s) - ld(tin, u - 1, s))
                    a6 = ld(sl, u, s) * (ld(tin, u, s + 1) - ld(tin, u, s - 1))
                    g = ((a1 + a2) + (a3 + a4)) + ((a5 + a6) + ld(zin, u, s)) + (left(q) - right(q))
                    parts0[u] = add(parts0[u], clip(val * g, span))
                    if k < 2:
                        nxt = g * ld(box.inv, u, s)
                        box.v[k + 1][at] = nxt
                        up, down = left(nxt), right(nxt)
                        tout[at] = up - down
                        zout[at] = ld(box.fl, u, s) * up + ld(box.fr, u, s) * down
                        parts1[u] = add(parts1[u], clip(nxt * g, span))
            acc0, acc1 = accs
            return gather(box, m, acc0, parts0, inner), gather(box, m, acc1, parts1, inner)

        tin, zin, tout, zout = box.t[k] + (box.t[k + 1] if k < 2 else (None, None))
        return run(loop, body, accs)

    def extract(base, count, unroll):
        def body(m, c):
            for src, dst in ((e_lab, k_lab), (e_b, k_b)):
                plane = jnp.concatenate([src[base + m], jnp.zeros((128 - PY, 128), src.dtype)], axis=0)
                turned = plane.T
                dst[pl.ds(4 * PX + base + m, 8, stride=PX), :] = turned[0:8]
                dst[pl.ds(LAYERS * PX + base + m, 8, stride=PX), :] = turned[120:128]
            return c
        lax.fori_loop(0, count, body, 0, unroll=unroll)

    own_rows = [W + 8 * i for i in range(Y // 8)]
    sigma(E, (W, 4, X // 4, 4), own_rows)
    arrive(lambda dx, dy: dx == 0)
    sigma(E, (W, 4, X // 4, 4), [0, PY - 8])
    extract(W, X, 4)
    s0 = diagonal(E, (W + 1, 3, (X - 2) // 3, 3), None, zero)
    s12 = apply(E, 0, (W + 2, 4, (X - 4) // 4, 4), None, (zero, zero))

    arrive(lambda dx, dy: dx != 0)
    extract(0, W, 4)
    extract(W + X, W, 4)
    sigma(E, (0, X + W, 2, 4), row_groups(0, PY))
    for field in (0, 1):
        for up in (0, 1):
            @pl.when(has[up])
            def _():
                phase2(up, field).start()

    s0 = diagonal(E, (1, X + 2, 2, 4), "ask", s0)
    s12 = apply(E, 0, (2, X, 2, 4), "ask", s12)
    s34 = apply(E, 1, (2, 4, (X + 4) // 4, 4), "ask", (zero, zero))
    s5, _ = apply(E, 2, (W, 4, X // 4, 4), None, (zero, zero))
    e_sums = [s0, *s12, *s34, s5]

    for field in (0, 1):
        for up in (0, 1):
            @pl.when(has[1 - up])
            def _():
                phase2(up, field).wait_recv()
    sigma(K, (0, 4, LAYERS // 2, 4), row_groups(0, PX))
    s0 = diagonal(K, (1, LAYERS, 2, 10), (3, 4, 5, 6), zero)
    s12 = apply(K, 0, (2, LAYERS, 2, 8), (2, 3, 4, 5), (zero, zero))
    s34 = apply(K, 1, (3, LAYERS, 2, 6), (1, 2, 3, 4), (zero, zero))
    s5, _ = apply(K, 2, (4, LAYERS, 2, 4), None, (zero, zero))
    k_sums = [s0, *s12, *s34, s5]

    edge = (lane < 4) | (lane >= 124)
    blocks = -(-X // 16)

    def complete():
        for k in range(3):
            for j in range(4):
                kint[pl.ds(j, X, stride=8), :] = K.v[k][pl.ds((LAYERS + 4 + j) * PX + W, X), :]
                kint[pl.ds(4 + j, X, stride=8), :] = K.v[k][pl.ds((4 + j) * PX + W, X), :]
            for q in range(blocks):
                kt[k, q] = kint[128 * q:128 * q + 128, :].T

        def body(m, c):
            for k in range(3):
                for s in range(W, W + Y, 8):
                    turned = pltpu.roll(kt[k, m // 16, pl.ds(s, 8), :], lax.rem(252 - 8 * lax.rem(m, 16), 128), 1)
                    E.v[k][m + W, pl.ds(s, 8), :] = jnp.where(edge, turned, E.v[k][m + W, pl.ds(s, 8), :])
            return c
        lax.fori_loop(0, X, body, 0, unroll=2)

    wide = lane[0:1]
    row = jnp.zeros((1, 128), jnp.float32)
    for k in range(6):
        from_k = jnp.where((wide >= W) & (wide < W + Y), jnp.sum(k_sums[k], axis=0, keepdims=True), 0.0)
        from_e = jnp.where((wide >= 4) & (wide < 124), jnp.sum(e_sums[k], axis=0, keepdims=True), 0.0)
        row = jnp.where(wide == k, jnp.sum(from_k + from_e, axis=1, keepdims=True), row)

    pl.semaphore_wait(greet.at[0], gxn - 1)
    slot = 0
    for stage, axes in enumerate(STAGES):
        ar[stage] = jnp.broadcast_to(row, (8, 128))
        copies = []
        first = slot
        for d in peers_of(axes):
            copy = pltpu.make_async_remote_copy(
                src_ref=ar.at[stage, pl.ds(0, 1), :], dst_ref=arslot.at[pl.ds(slot, 1), :], send_sem=sa.at[slot],
                recv_sem=ra.at[slot], device_id=peer(axes, d), device_id_type=MESH)
            copy.start()
            copies.append(copy)
            slot += 1
        if stage == 0:
            complete()
        for copy in copies:
            copy.wait_recv()
        row = row + jnp.sum(arslot[first:slot, :], axis=0, keepdims=True)
        for copy in copies:
            copy.wait_send()

    n = [jnp.broadcast_to(row[:, k:k + 1], (8, 128)) for k in range(6)]
    a = [n[k] - n[k + 1] for k in range(5)]
    safe = lambda num, den: jnp.where(den > 0, num / jnp.where(den > 0, den, 1.0), 0.0)
    l1, l2 = safe(a[1], a[0]), safe(a[2], a[0])
    d1 = a[2] - l1 * a[1]
    l21 = safe(a[3] - l1 * a[2], d1)
    d2 = a[4] - l2 * a[2] - l21 * (a[3] - l1 * a[2])
    y1 = n[1] - l1 * n[0]
    y2 = n[2] - l2 * n[0] - l21 * y1
    c2 = safe(y2, d2)
    c1 = safe(y1, d1) - l21 * c2
    c0 = safe(n[0], a[0]) - l1 * c1 - l2 * c2

    def finish(m, c):
        for s in range(0, Y, 8):
            out[m, pl.ds(s, 8), :] = (c0 * E.v[0][m + W, pl.ds(s + W, 8), :] + c1 * E.v[1][m + W, pl.ds(s + W, 8), :]
                                      + c2 * E.v[2][m + W, pl.ds(s + W, 8), :])
        return c

    lax.fori_loop(0, X, finish, 0, unroll=2)

    for field in (0, 1):
        for i, (dx, dy) in enumerate(DIRS):
            @pl.when(exists(dx, dy))
            def _():
                phase1(i, field).wait_send()
        for up in (0, 1):
            @pl.when(has[up])
            def _():
                phase2(up, field).wait_send()


def local(labels, conductivity, right_side, sizes):
    gxn, gyn, gzn = sizes
    X, Y, Z = labels.shape
    assert Z == 128 and Y % 8 == 0
    PX, PY = X + 2 * W, Y + 2 * W
    krows = 2 * LAYERS * PX
    f32 = jnp.float32
    count = {"gx": gxn, "gy": gyn, "gz": gzn}
    slots = sum(math.prod(count[a] for a in axes) - 1 for axes in STAGES)
    dma = pltpu.SemaphoreType.DMA
    return pl.pallas_call(
        functools.partial(kernel, (gxn, gyn, gzn, X, Y)),
        out_shape=jax.ShapeDtypeStruct((X, Y, Z), f32),
        in_specs=[
            pl.BlockSpec(memory_space=pltpu.SMEM),
            pl.BlockSpec(memory_space=pl.ANY),
            pl.BlockSpec(memory_space=pl.ANY),
        ],
        out_specs=pl.BlockSpec(memory_space=pltpu.VMEM),
        scratch_shapes=[
            pltpu.VMEM((PX, PY, 128), jnp.int32),
            pltpu.VMEM((PX, PY, 128), f32),
            pltpu.VMEM((21, PX, PY, 128), f32),
            pltpu.VMEM((krows, 128), jnp.int32),
            pltpu.VMEM((krows, 128), f32),
            pltpu.VMEM((21, krows, 128), f32),
            pltpu.VMEM((-(-X // 16) * 128, 128), f32),
            pltpu.VMEM((3, -(-X // 16), 128, 128), f32),
            pltpu.VMEM((3, 8, 128), f32),
            pltpu.VMEM((slots, 128), f32),
            dma((2,)), dma((8, 2)), dma((8, 2)), dma((2, 2)), dma((2, 2)), dma((slots,)), dma((slots,)),
            pltpu.SemaphoreType.REGULAR((2,)),
        ],
        compiler_params=pltpu.CompilerParams(
            collective_id=0, has_side_effects=True, vmem_limit_bytes=62 * 1024 * 1024),
    )(conductivity, labels, right_side)


def solution(mesh):
    sizes = (mesh.shape["gx"], mesh.shape["gy"], mesh.shape["gz"])
    spec = P("gx", "gy", "gz")
    return jax.shard_map(
        functools.partial(local, sizes=sizes), mesh=mesh, in_specs=(spec, P(), spec), out_specs=spec, check_vma=False)
```

```python
import functools
import itertools
import math

import jax
import jax.numpy as jnp
from jax import lax
from jax.experimental import pallas as pl
from jax.experimental.pallas import tpu as pltpu
from jax.sharding import PartitionSpec as P

MESH = pl.DeviceIdType.MESH
W = 4
LAYERS = 12
SKEW = 8
OUTSIDE = 8
DIRS = ((0, -1), (0, 1), (-1, 0), (1, 0), (-1, -1), (-1, 1), (1, -1), (1, 1))
STAGES = (("gx", "gy"), ("gz",))


def row_groups(lo, hi):
    starts = list(range(lo, hi - 7, 8))
    if starts[-1] + 8 < hi:
        starts.append(hi - 8)
    return starts


def group_spans(lo, hi, first, last):
    spans, done = [], first
    for start in row_groups(lo, hi):
        low, high = max(done, start), min(last, start + 8)
        done = max(done, high)
        spans.append((start, low - start, max(high, low) - start))
    return spans


def kernel(sizes, cond_hbm, lab_hbm, b_hbm, out_any, *scr):
    (gxn, gyn, gzn, X, Y) = sizes
    PX, PY = X + 2 * W, Y + 2 * W
    KX = PX + 1
    (e_lab, e_b, e_arr, k_lab, k_b, k_arr, kint, kt, ar, arslot,
     load_sem, s1, r1, s2, r2, sa, ra, greet, out, out_sem, cond) = scr
    gx, gy, gz = lax.axis_index("gx"), lax.axis_index("gy"), lax.axis_index("gz")

    load_lab = pltpu.make_async_copy(lab_hbm, e_lab.at[pl.ds(W, X), pl.ds(W, Y), :], load_sem.at[0])
    load_b = pltpu.make_async_copy(b_hbm, e_b.at[pl.ds(W, X), pl.ds(W, Y), :], load_sem.at[1])
    load_cond = pltpu.make_async_copy(cond_hbm, cond, load_sem.at[2])
    load_cond.start()
    load_lab.start()
    load_b.start()

    def exists(dx, dy):
        ok = None
        for pos, d, n in ((gx, dx, gxn), (gy, dy, gyn)):
            if d:
                here = (pos + d >= 0) & (pos + d < n)
                ok = here if ok is None else ok & here
        return ok

    ring = {"gx": (gx, gxn), "gy": (gy, gyn), "gz": (gz, gzn)}

    def peers_of(axes):
        return [d for d in itertools.product(*[range(ring[a][1]) for a in axes]) if any(d)]

    def peer(axes, d):
        return {a: lax.rem(ring[a][0] + k, ring[a][1]) for a, k in zip(axes, d) if k}

    barrier = pltpu.get_barrier_semaphore()
    count = 0
    for axis in ("gy", "gx", "gz"):
        for d in peers_of((axis,)):
            pl.semaphore_signal(barrier, inc=1, device_id=peer((axis,), d), device_id_type=MESH)
            count = count + 1
    for dx, dy in DIRS:
        if dx and dy:
            ok = exists(dx, dy)

            @pl.when(ok)
            def _():
                pl.semaphore_signal(barrier, inc=1, device_id={"gx": gx + dx, "gy": gy + dy}, device_id_type=MESH)

            count = count + ok.astype(jnp.int32)
    pl.semaphore_wait(barrier, count)

    def pass_on(i, axis):
        for d in peers_of((axis,)):
            pl.semaphore_signal(greet.at[i], inc=1, device_id=peer((axis,), d), device_id_type=MESH)

    pass_on(0, "gx")

    def region(d, n, width, arriving):
        if d == 0:
            return pl.ds(W, n)
        if arriving:
            return pl.ds(W + n, width) if d < 0 else pl.ds(W - width, width)
        return pl.ds(W, width) if d < 0 else pl.ds(W + n - width, width)

    def phase1(i, field):
        dx, dy = DIRS[i]
        ref, width = ((e_lab, W), (e_b, W - 1))[field]
        src = ref.at[region(dx, X, width, False), region(dy, Y, width, False), :]
        dst = ref.at[region(dx, X, width, True), region(dy, Y, width, True), :]
        target = {}
        if dx:
            target["gx"] = jnp.clip(gx + dx, 0, gxn - 1)
        if dy:
            target["gy"] = jnp.clip(gy + dy, 0, gyn - 1)
        return pltpu.make_async_remote_copy(
            src_ref=src, dst_ref=dst, send_sem=s1.at[i, field], recv_sem=r1.at[i, field],
            device_id=target, device_id_type=MESH)

    for field, load in ((0, load_lab), (1, load_b)):
        load.wait()
        for i, (dx, dy) in enumerate(DIRS):
            @pl.when(exists(dx, dy))
            def _():
                phase1(i, field).start()

    def fill_e(xs, nx, ys, ny):
        def body(m, c):
            e_lab[xs + m, pl.ds(ys, ny), :] = jnp.full((ny, 128), OUTSIDE, jnp.int32)
            e_b[xs + m, pl.ds(ys, ny), :] = jnp.zeros((ny, 128), jnp.float32)
            return c
        lax.fori_loop(0, nx, body, 0)

    @pl.when(gx == 0)
    def _():
        fill_e(0, W, 0, PY)

    @pl.when(gx == gxn - 1)
    def _():
        fill_e(W + X, W, 0, PY)

    @pl.when(gy == 0)
    def _():
        fill_e(0, PX, 0, W)

    @pl.when(gy == gyn - 1)
    def _():
        fill_e(0, PX, W + Y, W)

    def fill_k(side, layer):
        rows = pl.ds((side * LAYERS + layer) * KX, W * KX)
        k_lab[rows, :] = jnp.full((W * KX, 128), OUTSIDE, jnp.int32)
        k_b[rows, :] = jnp.zeros((W * KX, 128), jnp.float32)

    @pl.when(gz == 0)
    def _():
        fill_k(0, 0)

    @pl.when(gz == gzn - 1)
    def _():
        fill_k(1, 2 * W)

    def arrive(pick):
        for field in (0, 1):
            for i, (dx, dy) in enumerate(DIRS):
                if pick(dx, dy):
                    @pl.when(exists(-dx, -dy))
                    def _():
                        phase1(i, field).wait_recv()

    def phase2(up, field):
        ref, width = ((k_lab, W), (k_b, W - 1))[field]
        if up:
            src, dst = LAYERS + 8 - width, W - width
        else:
            src, dst = W, LAYERS + 8
        target = {"gz": jnp.clip(gz + (1 if up else -1), 0, gzn - 1)}
        return pltpu.make_async_remote_copy(
            src_ref=ref.at[pl.ds(src * KX, width * KX), :], dst_ref=ref.at[pl.ds(dst * KX, width * KX), :],
            send_sem=s2.at[up, field], recv_sem=r2.at[up, field], device_id=target, device_id_type=MESH)

    has = (gz > 0, gz < gzn - 1)

    load_cond.wait()
    sub = lax.broadcasted_iota(jnp.int32, (8, 128), 0)
    lane = lax.broadcasted_iota(jnp.int32, (8, 128), 1)
    factor = (0.5, 0.5, 0.5, 0.25, 0.25, 0.25, 1.0)
    tables = []
    for c in range(7):
        tab = jnp.zeros((8, 128), jnp.float32)
        for label in range(8):
            tab = jnp.where(sub == label, cond[c, label], tab)
        tables.append(tab * factor[c])

    def lookup(lab, picks):
        inside = lab < OUTSIDE
        index = jnp.bitwise_and(lab, 7)
        return [jnp.where(inside, jnp.take_along_axis(tables[k], index, axis=0, mode="promise_in_bounds"), 0.0)
                for k in picks]

    class Box:
        pass

    class Field:
        def __init__(self, ref, base, height):
            self.ref, self.base, self.height = ref, base, height

        def rows(self, m, s, n=8):
            return pl.ds(self.base + m * self.height + s, n), slice(None)

        def __getitem__(self, at):
            return self.ref[self.rows(*at)]

        def __setitem__(self, at, val):
            self.ref[self.rows(*at)] = val

    class Block(Field):
        def rows(self, m, s):
            return m, pl.ds(s, 8), slice(None)

    E, K = Box(), Box()
    E.lab, E.b = Block(e_lab, 0, PY), Block(e_b, 0, PY)
    K.lab, K.b = Field(k_lab, 0, KX), Field(k_b, 0, KX)
    E.arrays = [Field(e_arr, c * (PX * PY + SKEW), PY) for c in range(18)]
    K.arrays = [Field(k_arr, c * (2 * LAYERS * KX + SKEW), KX) for c in range(18)]
    for box in (E, K):
        a = box.arrays
        box.sig = a[:6]
        box.fm, box.fs, box.cpp, box.cpm, box.inv = a[6:11]
        box.v = a[11:14]
        box.t = [(a[14], a[15]), (a[16], a[17]), (a[14], a[15])]
    E.names, K.names = (0, 1, 2, 3, 4, 5), (2, 0, 1, 4, 5, 3)
    E.span, K.span = Y, X
    K.inner = lambda m: ((m >= 4) & (m < 8)) | ((m >= LAYERS + 4) & (m < LAYERS + 8))
    E.inner = lambda m: (m >= W) & (m < W + X)
    zero = jnp.zeros((8, 128), jnp.float32)
    left = lambda t: pltpu.roll(t, 127, 1)
    right = lambda t: pltpu.roll(t, 1, 1)

    class Cells:
        def __init__(self, box, m):
            self.box, self.m, self.seen = box, m, {}

        def __call__(self, ref, dm, s):
            key = (id(ref), dm, s)
            if key not in self.seen:
                self.seen[key] = ref[self.m + dm, s]
            return self.seen[key]

    def run(loop, body, init):
        base, stride, trips, _ = loop
        start = base if callable(base) else lambda t: base + t * stride
        return lax.fori_loop(0, trips, lambda t, c: body(start(t), c), init)

    def spans(box, halo):
        return group_spans(W - halo, W + box.span + halo, W, W + box.span)

    def clip(val, span):
        _, low, high = span
        if low >= high:
            return None
        if (low, high) != (0, 8):
            val = jnp.where((sub >= low) & (sub < high), val, 0.0)
        return val

    def add(total, val):
        return val if total is None else total if val is None else total + val

    def gather(box, m, acc, parts, inner):
        for u, part in enumerate(parts):
            if part is not None and (inner is None or inner == "ask" or u in inner):
                acc = acc + (jnp.where(box.inner(m + u), part, 0.0) if inner == "ask" else part)
        return acc

    def sigma(box, loop, starts):
        def body(m, c):
            for s in starts:
                for u in range(loop[3]):
                    sig = lookup(box.lab[m + u, s], range(6))
                    for k in range(6):
                        box.sig[k][m + u, s] = sig[k]
            return c
        run(loop, body, 0)

    def spread(box, k, m, s, v):
        up, down = left(v), right(v)
        box.t[k][0][m, s] = up - down
        box.t[k][1][m, s] = up + down

    def diagonal(box, loop, inner, acc):
        sm, ss, sl, ms = [box.sig[box.names[i]] for i in range(4)]

        def body(m, acc):
            ld = Cells(box, m)
            parts = [None] * loop[3]
            for span in spans(box, 3):
                s = span[0]
                for u in range(loop[3]):
                    at = (m + u, s)
                    cm, cs, cl, cx = ld(sm, u, s), ld(ss, u, s), ld(sl, u, s), ld(ms, u, s)
                    fm, fs = cm + ld(sm, u + 1, s), cs + ld(ss, u, s + 1)
                    lab = ld(box.lab, u, s)
                    total = (lookup(lab, (6,))[0] + fm + (cm + ld(sm, u - 1, s))) + (fs + (cs + ld(ss, u, s - 1)))
                    total = total + ((cl + cl) + (left(cl) + right(cl)))
                    inv = jnp.where(lab < OUTSIDE, 1.0 / total, 0.0)
                    b = ld(box.b, u, s)
                    v0 = b * inv
                    box.fm[at], box.fs[at] = fm, fs
                    box.cpp[at] = cx + ld(ms, u + 1, s + 1)
                    box.cpm[at] = -(cx + ld(ms, u + 1, s - 1))
                    box.inv[at] = inv
                    box.v[0][at] = v0
                    spread(box, 0, m + u, s, v0)
                    parts[u] = add(parts[u], clip(b * v0, span))
            return gather(box, m, acc, parts, inner)
        return run(loop, body, acc)

    def apply(box, k, loop, inner, accs):
        v, lx, ml, sl = box.v[k], box.sig[box.names[2]], box.sig[box.names[4]], box.sig[box.names[5]]

        def body(m, accs):
            ld = Cells(box, m)
            parts0, parts1 = [None] * loop[3], [None] * loop[3]
            for span in spans(box, 2 - k):
                s = span[0]
                for u in range(loop[3]):
                    at = (m + u, s)
                    val, hi, lo = ld(v, u, s), ld(v, u + 1, s), ld(v, u - 1, s)
                    up, down = ld(v, u, s + 1), ld(v, u, s - 1)
                    a1 = ld(box.fm, u, s) * hi + ld(box.fm, u - 1, s) * lo
                    a2 = ld(box.fs, u, s) * up + ld(box.fs, u, s - 1) * down
                    a3 = ld(box.cpp, u, s) * ld(v, u + 1, s + 1) + ld(box.cpp, u - 1, s - 1) * ld(v, u - 1, s - 1)
                    a4 = ld(box.cpm, u, s) * ld(v, u + 1, s - 1) + ld(box.cpm, u - 1, s + 1) * ld(v, u - 1, s + 1)
                    q = (ld(ml, u + 1, s) * hi - ld(ml, u - 1, s) * lo) + (
                        ld(sl, u, s + 1) * up - ld(sl, u, s - 1) * down)
                    a5 = ld(ml, u, s) * (ld(tin, u + 1, s) - ld(tin, u - 1, s))
                    a6 = ld(sl, u, s) * (ld(tin, u, s + 1) - ld(tin, u, s - 1))
                    c = ld(lx, u, s)
                    p = c * val
                    g = ((a1 + a2) + (a3 + a4)) + ((a5 + a6) + c * ld(zin, u, s)) + (left(p + q) + right(p - q))
                    parts0[u] = add(parts0[u], clip(val * g, span))
                    if k < 2:
                        nxt = g * ld(box.inv, u, s)
                        box.v[k + 1][at] = nxt
                        spread(box, k + 1, m + u, s, nxt)
                        parts1[u] = add(parts1[u], clip(nxt * g, span))
            acc0, acc1 = accs
            return gather(box, m, acc0, parts0, inner), gather(box, m, acc1, parts1, inner)

        tin, zin = box.t[k]
        return run(loop, body, accs)

    def extract(plane, trips):
        mine = [jnp.right_shift(lane, 4) == p for p in range(8)]

        def body(t, c):
            for src, dst in ((E.lab, k_lab), (E.b, k_b)):
                tiles = []
                for s in range(0, PY, 8):
                    tile = pltpu.roll(src[plane(t, 0), s], 8, 1)
                    for p in range(1, 8):
                        tile = jnp.where(mine[p], pltpu.roll(src[plane(t, p), s], (8 + 16 * p) % 128, 1), tile)
                    tiles.append(tile)
                tiles.append(jnp.zeros((128 - PY, 128), tile.dtype))
                turned = jnp.concatenate(tiles, axis=0).T
                for p in range(8):
                    x = plane(t, p)
                    dst[pl.ds(LAYERS * KX + x, 8, stride=KX), :] = turned[16 * p:16 * p + 8]
                    dst[pl.ds(4 * KX + x, 8, stride=KX), :] = turned[16 * p + 8:16 * p + 16]
            return c
        lax.fori_loop(0, trips, body, 0)

    own_rows = [W + 8 * i for i in range(Y // 8)]
    sigma(E, (W, 4, X // 4, 4), own_rows)
    arrive(lambda dx, dy: dx == 0)
    sigma(E, (W, 4, X // 4, 4), [0, PY - 8])
    extract(lambda t, p: W + 8 * t + p, X // 8)
    s0 = diagonal(E, (W + 1, 3, (X - 2) // 3, 3), None, zero)
    s12 = apply(E, 0, (W + 2, 4, (X - 4) // 4, 4), None, (zero, zero))

    arrive(lambda dx, dy: dx != 0)
    extract(lambda t, p: p + p // W * X, 1)
    sigma(E, (0, X + W, 2, 4), row_groups(0, PY))
    for field in (0, 1):
        for up in (0, 1):
            @pl.when(has[up])
            def _():
                phase2(up, field).start()

    s0 = diagonal(E, (1, X + 2, 2, 4), "ask", s0)
    s12 = apply(E, 0, (2, X, 2, 4), "ask", s12)
    s34 = apply(E, 1, (2, 4, (X + 4) // 4, 4), "ask", (zero, zero))
    s5, _ = apply(E, 2, (W, 4, X // 4, 4), None, (zero, zero))
    e_sums = [s0, *s12, *s34, s5]

    for field in (0, 1):
        for up in (0, 1):
            @pl.when(has[1 - up])
            def _():
                phase2(up, field).wait_recv()
    sigma(K, (0, 4, LAYERS // 2, 4), row_groups(0, PX))
    s0 = diagonal(K, (lambda t: 1 + 2 * t + (t // 5) * 2, 0, 10, 2), "ask", zero)
    s12 = apply(K, 0, (lambda t: 2 + 4 * t + (t // 2) * 4, 0, 4, 4), "ask", (zero, zero))
    s34 = apply(K, 1, (lambda t: 3 + 3 * t + (t // 2) * 6, 0, 4, 3), "ask", (zero, zero))
    s5, _ = apply(K, 2, (4, LAYERS, 2, 4), None, (zero, zero))
    k_sums = [s0, *s12, *s34, s5]

    edge = (lane < 4) | (lane >= 124)
    blocks = -(-X // 16)

    def complete():
        for k in range(3):
            for j in range(4):
                kint[pl.ds(j, X, stride=8), :] = k_arr[K.v[k].rows(LAYERS + 4 + j, W, X)]
                kint[pl.ds(4 + j, X, stride=8), :] = k_arr[K.v[k].rows(4 + j, W, X)]
            for q in range(blocks):
                kt[k, q] = kint[128 * q:128 * q + 128, :].T

        def body(m, c):
            for k in range(3):
                for s in range(W, W + Y, 8):
                    turned = pltpu.roll(kt[k, m // 16, pl.ds(s, 8), :], lax.rem(252 - 8 * lax.rem(m, 16), 128), 1)
                    E.v[k][m + W, s] = jnp.where(edge, turned, E.v[k][m + W, s])
            return c
        lax.fori_loop(0, X, body, 0, unroll=2)

    wide = lane[0:1]
    row = jnp.zeros((1, 128), jnp.float32)
    for k in range(6):
        from_k = jnp.where((wide >= W) & (wide < W + Y), jnp.sum(k_sums[k], axis=0, keepdims=True), 0.0)
        from_e = jnp.where((wide >= 4) & (wide < 124), jnp.sum(e_sums[k], axis=0, keepdims=True), 0.0)
        row = jnp.where(wide == k, jnp.sum(from_k + from_e, axis=1, keepdims=True), row)

    pl.semaphore_wait(greet.at[0], gxn - 1)
    slot = 0
    for stage, axes in enumerate(STAGES):
        ar[stage] = jnp.broadcast_to(row, (8, 128))
        copies = []
        first = slot
        for d in peers_of(axes):
            copy = pltpu.make_async_remote_copy(
                src_ref=ar.at[stage, pl.ds(0, 1), :], dst_ref=arslot.at[pl.ds(slot, 1), :], send_sem=sa.at[slot],
                recv_sem=ra.at[slot], device_id=peer(axes, d), device_id_type=MESH)
            copy.start()
            copies.append(copy)
            slot += 1
        if stage == 0:
            complete()
        for copy in copies:
            copy.wait_recv()
        row = row + jnp.sum(arslot[first:slot, :], axis=0, keepdims=True)
        for copy in copies:
            copy.wait_send()

    n = [jnp.broadcast_to(row[:, k:k + 1], (8, 128)) for k in range(6)]
    a = [n[k] - n[k + 1] for k in range(5)]
    safe = lambda num, den: jnp.where(den > 0, num / jnp.where(den > 0, den, 1.0), 0.0)
    l1, l2 = safe(a[1], a[0]), safe(a[2], a[0])
    d1 = a[2] - l1 * a[1]
    l21 = safe(a[3] - l1 * a[2], d1)
    d2 = a[4] - l2 * a[2] - l21 * (a[3] - l1 * a[2])
    y1 = n[1] - l1 * n[0]
    y2 = n[2] - l2 * n[0] - l21 * y1
    c2 = safe(y2, d2)
    c1 = safe(y1, d1) - l21 * c2
    c0 = safe(n[0], a[0]) - l1 * c1 - l2 * c2

    quarter = X // 4

    def put(t):
        part = pl.ds(t * quarter, quarter)
        return pltpu.make_async_copy(out.at[part], out_any.at[part], out_sem.at[t])

    def finish(t, c):
        for u in range(2):
            m = 2 * t + u
            for s in range(0, Y, 8):
                out[m, pl.ds(s, 8), :] = (c0 * E.v[0][m + W, s + W] + c1 * E.v[1][m + W, s + W]
                                          + c2 * E.v[2][m + W, s + W])
        return c

    def chunk(t, c):
        lax.fori_loop(t * (quarter // 2), (t + 1) * (quarter // 2), finish, 0)
        put(t).start()
        return c

    lax.fori_loop(0, 4, chunk, 0)

    for field in (0, 1):
        for i, (dx, dy) in enumerate(DIRS):
            @pl.when(exists(dx, dy))
            def _():
                phase1(i, field).wait_send()
        for up in (0, 1):
            @pl.when(has[up])
            def _():
                phase2(up, field).wait_send()

    for t in range(4):
        put(t).wait()


def local(labels, conductivity, right_side, sizes):
    gxn, gyn, gzn = sizes
    X, Y, Z = labels.shape
    assert Z == 128 and Y % 8 == 0
    PX, PY = X + 2 * W, Y + 2 * W
    krows = 2 * LAYERS * (PX + 1)
    f32 = jnp.float32
    count = {"gx": gxn, "gy": gyn, "gz": gzn}
    slots = sum(math.prod(count[a] for a in axes) - 1 for axes in STAGES)
    dma = pltpu.SemaphoreType.DMA
    return pl.pallas_call(
        functools.partial(kernel, (gxn, gyn, gzn, X, Y)),
        out_shape=jax.ShapeDtypeStruct((X, Y, Z), f32),
        in_specs=[
            pl.BlockSpec(memory_space=pltpu.HBM),
            pl.BlockSpec(memory_space=pltpu.HBM),
            pl.BlockSpec(memory_space=pltpu.HBM),
        ],
        out_specs=pl.BlockSpec(memory_space=pl.ANY),
        scratch_shapes=[
            pltpu.VMEM((PX, PY, 128), jnp.int32),
            pltpu.VMEM((PX, PY, 128), f32),
            pltpu.VMEM((18 * (PX * PY + SKEW), 128), f32),
            pltpu.VMEM((krows, 128), jnp.int32),
            pltpu.VMEM((krows, 128), f32),
            pltpu.VMEM((18 * (krows + SKEW), 128), f32),
            pltpu.VMEM((-(-X // 16) * 128, 128), f32),
            pltpu.VMEM((3, -(-X // 16), 128, 128), f32),
            pltpu.VMEM((3, 8, 128), f32),
            pltpu.VMEM((slots, 128), f32),
            dma((3,)), dma((8, 2)), dma((8, 2)), dma((2, 2)), dma((2, 2)), dma((slots,)), dma((slots,)),
            pltpu.SemaphoreType.REGULAR((2,)), pltpu.VMEM((X, Y, Z), f32), dma((4,)),
            pltpu.SMEM((7, 8), f32),
        ],
        compiler_params=pltpu.CompilerParams(
            collective_id=0, has_side_effects=True, vmem_limit_bytes=62 * 1024 * 1024),
    )(conductivity, labels, right_side)


def solution(mesh):
    sizes = (mesh.shape["gx"], mesh.shape["gy"], mesh.shape["gz"])
    spec = P("gx", "gy", "gz")
    return jax.shard_map(
        functools.partial(local, sizes=sizes), mesh=mesh, in_specs=(spec, P(), spec), out_specs=spec, check_vma=False)
```

```python
import functools
import itertools
import math

import jax
import jax.numpy as jnp
from jax import lax
from jax.experimental import pallas as pl
from jax.experimental.pallas import tpu as pltpu
from jax.sharding import PartitionSpec as P

MESH = pl.DeviceIdType.MESH
W = 4
LAYERS = 12
SKEW = 8
OUTSIDE = 8
DIRS = ((0, -1), (0, 1), (-1, 0), (1, 0), (-1, -1), (-1, 1), (1, -1), (1, 1))
STAGES = (("gy",), ("gx", "gz"))


def row_groups(lo, hi):
    starts = list(range(lo, hi - 7, 8))
    if starts[-1] + 8 < hi:
        starts.append(hi - 8)
    return starts


def group_spans(lo, hi, first, last):
    spans, done = [], first
    for start in row_groups(lo, hi):
        low, high = max(done, start), min(last, start + 8)
        done = max(done, high)
        spans.append((start, low - start, max(high, low) - start))
    return spans


def kernel(sizes, cond_hbm, lab_hbm, b_hbm, out_any, *scr):
    (gxn, gyn, gzn, X, Y) = sizes
    PX, PY = X + 2 * W, Y + 2 * W
    KX = PX + 1
    (e_lab, e_b, e_arr, k_lab, k_b, k_arr, kint, kt, ar, arslot,
     load_sem, s1, r1, s2, r2, sa, ra, greet, out, out_sem, cond) = scr
    gx, gy, gz = lax.axis_index("gx"), lax.axis_index("gy"), lax.axis_index("gz")

    load_lab = pltpu.make_async_copy(lab_hbm, e_lab.at[pl.ds(W, X), pl.ds(W, Y), :], load_sem.at[0])
    load_b = pltpu.make_async_copy(b_hbm, e_b.at[pl.ds(W, X), pl.ds(W, Y), :], load_sem.at[1])
    load_cond = pltpu.make_async_copy(cond_hbm, cond, load_sem.at[2])
    load_cond.start()
    load_lab.start()
    load_b.start()

    def exists(dx, dy):
        ok = None
        for pos, d, n in ((gx, dx, gxn), (gy, dy, gyn)):
            if d:
                here = (pos + d >= 0) & (pos + d < n)
                ok = here if ok is None else ok & here
        return ok

    ring = {"gx": (gx, gxn), "gy": (gy, gyn), "gz": (gz, gzn)}

    def peers_of(axes):
        far = lambda d: sum(min(k, ring[a][1] - k) for a, k in zip(axes, d))
        return sorted((d for d in itertools.product(*[range(ring[a][1]) for a in axes]) if any(d)), key=far, reverse=True)

    def peer(axes, d):
        return {a: lax.rem(ring[a][0] + k, ring[a][1]) for a, k in zip(axes, d) if k}

    barrier = pltpu.get_barrier_semaphore()
    count = 0
    for axis in ("gy", "gx", "gz"):
        for d in peers_of((axis,)):
            pl.semaphore_signal(barrier, inc=1, device_id=peer((axis,), d), device_id_type=MESH)
            count = count + 1
    for dx, dy in DIRS:
        if dx and dy:
            ok = exists(dx, dy)

            @pl.when(ok)
            def _():
                pl.semaphore_signal(barrier, inc=1, device_id={"gx": gx + dx, "gy": gy + dy}, device_id_type=MESH)

            count = count + ok.astype(jnp.int32)
    pl.semaphore_wait(barrier, count)

    def pass_on(i, axis):
        for d in peers_of((axis,)):
            pl.semaphore_signal(greet.at[i], inc=1, device_id=peer((axis,), d), device_id_type=MESH)

    pass_on(0, "gx")

    def region(d, n, width, arriving):
        if d == 0:
            return pl.ds(W, n)
        if arriving:
            return pl.ds(W + n, width) if d < 0 else pl.ds(W - width, width)
        return pl.ds(W, width) if d < 0 else pl.ds(W + n - width, width)

    def phase1(i, field):
        dx, dy = DIRS[i]
        ref, width = ((e_lab, W), (e_b, W - 1))[field]
        src = ref.at[region(dx, X, width, False), region(dy, Y, width, False), :]
        dst = ref.at[region(dx, X, width, True), region(dy, Y, width, True), :]
        target = {}
        if dx:
            target["gx"] = jnp.clip(gx + dx, 0, gxn - 1)
        if dy:
            target["gy"] = jnp.clip(gy + dy, 0, gyn - 1)
        return pltpu.make_async_remote_copy(
            src_ref=src, dst_ref=dst, send_sem=s1.at[i, field], recv_sem=r1.at[i, field],
            device_id=target, device_id_type=MESH)

    for field, load in ((0, load_lab), (1, load_b)):
        load.wait()
        for i, (dx, dy) in enumerate(DIRS):
            @pl.when(exists(dx, dy))
            def _():
                phase1(i, field).start()

    def fill_e(xs, nx, ys, ny):
        def body(m, c):
            e_lab[xs + m, pl.ds(ys, ny), :] = jnp.full((ny, 128), OUTSIDE, jnp.int32)
            e_b[xs + m, pl.ds(ys, ny), :] = jnp.zeros((ny, 128), jnp.float32)
            return c
        lax.fori_loop(0, nx, body, 0)

    @pl.when(gx == 0)
    def _():
        fill_e(0, W, 0, PY)

    @pl.when(gx == gxn - 1)
    def _():
        fill_e(W + X, W, 0, PY)

    @pl.when(gy == 0)
    def _():
        fill_e(0, PX, 0, W)

    @pl.when(gy == gyn - 1)
    def _():
        fill_e(0, PX, W + Y, W)

    def fill_k(side, layer):
        rows = pl.ds((side * LAYERS + layer) * KX, W * KX)
        k_lab[rows, :] = jnp.full((W * KX, 128), OUTSIDE, jnp.int32)
        k_b[rows, :] = jnp.zeros((W * KX, 128), jnp.float32)

    @pl.when(gz == 0)
    def _():
        fill_k(0, 0)

    @pl.when(gz == gzn - 1)
    def _():
        fill_k(1, 2 * W)

    def arrive(pick):
        for field in (0, 1):
            for i, (dx, dy) in enumerate(DIRS):
                if pick(dx, dy):
                    @pl.when(exists(-dx, -dy))
                    def _():
                        phase1(i, field).wait_recv()

    def phase2(up, field):
        ref, width = ((k_lab, W), (k_b, W - 1))[field]
        if up:
            src, dst = LAYERS + 8 - width, W - width
        else:
            src, dst = W, LAYERS + 8
        target = {"gz": jnp.clip(gz + (1 if up else -1), 0, gzn - 1)}
        return pltpu.make_async_remote_copy(
            src_ref=ref.at[pl.ds(src * KX, width * KX), :], dst_ref=ref.at[pl.ds(dst * KX, width * KX), :],
            send_sem=s2.at[up, field], recv_sem=r2.at[up, field], device_id=target, device_id_type=MESH)

    has = (gz > 0, gz < gzn - 1)

    load_cond.wait()
    sub = lax.broadcasted_iota(jnp.int32, (8, 128), 0)
    lane = lax.broadcasted_iota(jnp.int32, (8, 128), 1)
    factor = (0.5, 0.5, 0.5, 0.25, 0.25, 0.25, 1.0)
    tables = []
    for c in range(7):
        tab = jnp.zeros((8, 128), jnp.float32)
        for label in range(8):
            tab = jnp.where(sub == label, cond[c, label], tab)
        tables.append(tab * factor[c])

    def lookup(lab, picks):
        inside = lab < OUTSIDE
        index = jnp.bitwise_and(lab, 7)
        return [jnp.where(inside, jnp.take_along_axis(tables[k], index, axis=0, mode="promise_in_bounds"), 0.0)
                for k in picks]

    class Box:
        pass

    class Field:
        def __init__(self, ref, base, height):
            self.ref, self.base, self.height = ref, base, height

        def rows(self, m, s, n=8):
            return pl.ds(self.base + m * self.height + s, n), slice(None)

        def __getitem__(self, at):
            return self.ref[self.rows(*at)]

        def __setitem__(self, at, val):
            self.ref[self.rows(*at)] = val

    class Block(Field):
        def rows(self, m, s):
            return m, pl.ds(s, 8), slice(None)

    E, K = Box(), Box()
    E.lab, E.b = Block(e_lab, 0, PY), Block(e_b, 0, PY)
    K.lab, K.b = Field(k_lab, 0, KX), Field(k_b, 0, KX)
    E.arrays = [Field(e_arr, c * (PX * PY + SKEW), PY) for c in range(18)]
    K.arrays = [Field(k_arr, c * (2 * LAYERS * KX + SKEW), KX) for c in range(18)]
    for box in (E, K):
        a = box.arrays
        box.sig = a[:6]
        box.fm, box.fs, box.cpp, box.cpm, box.inv = a[6:11]
        box.v = a[11:14]
        box.t = [(a[14], a[15]), (a[16], a[17]), (a[14], a[15])]
    E.names, K.names = (0, 1, 2, 3, 4, 5), (2, 0, 1, 4, 5, 3)
    E.span, K.span = Y, X
    K.inner = lambda m: ((m >= 4) & (m < 8)) | ((m >= LAYERS + 4) & (m < LAYERS + 8))
    E.inner = lambda m: (m >= W) & (m < W + X)
    zero = jnp.zeros((8, 128), jnp.float32)
    left = lambda t: pltpu.roll(t, 127, 1)
    right = lambda t: pltpu.roll(t, 1, 1)

    class Cells:
        def __init__(self, box, m):
            self.box, self.m, self.seen = box, m, {}

        def __call__(self, ref, dm, s):
            key = (id(ref), dm, s)
            if key not in self.seen:
                self.seen[key] = ref[self.m + dm, s]
            return self.seen[key]

    def run(loop, body, init):
        base, stride, trips, _ = loop
        start = base if callable(base) else lambda t: base + t * stride
        return lax.fori_loop(0, trips, lambda t, c: body(start(t), c), init)

    def spans(box, halo):
        return group_spans(W - halo, W + box.span + halo, W, W + box.span)

    def clip(val, span):
        _, low, high = span
        if low >= high:
            return None
        if (low, high) != (0, 8):
            val = jnp.where((sub >= low) & (sub < high), val, 0.0)
        return val

    def add(total, val):
        return val if total is None else total if val is None else total + val

    def gather(box, m, acc, parts, inner):
        for u, part in enumerate(parts):
            if part is not None and (inner is None or inner == "ask" or u in inner):
                acc = acc + (jnp.where(box.inner(m + u), part, 0.0) if inner == "ask" else part)
        return acc

    def sigma(box, loop, starts):
        def body(m, c):
            for s in starts:
                for u in range(loop[3]):
                    sig = lookup(box.lab[m + u, s], range(6))
                    for k in range(6):
                        box.sig[k][m + u, s] = sig[k]
            return c
        run(loop, body, 0)

    def spread(box, k, m, s, v):
        up, down = left(v), right(v)
        box.t[k][0][m, s] = up - down
        box.t[k][1][m, s] = up + down

    def diagonal(box, loop, inner, acc):
        sm, ss, sl, ms = [box.sig[box.names[i]] for i in range(4)]

        def body(m, acc):
            ld = Cells(box, m)
            parts = [None] * loop[3]
            for span in spans(box, 3):
                s = span[0]
                for u in range(loop[3]):
                    at = (m + u, s)
                    cm, cs, cl, cx = ld(sm, u, s), ld(ss, u, s), ld(sl, u, s), ld(ms, u, s)
                    fm, fs = cm + ld(sm, u + 1, s), cs + ld(ss, u, s + 1)
                    lab = ld(box.lab, u, s)
                    total = (lookup(lab, (6,))[0] + fm + (cm + ld(sm, u - 1, s))) + (fs + (cs + ld(ss, u, s - 1)))
                    total = total + ((cl + cl) + (left(cl) + right(cl)))
                    inv = jnp.where(lab < OUTSIDE, 1.0 / total, 0.0)
                    b = ld(box.b, u, s)
                    v0 = b * inv
                    box.fm[at], box.fs[at] = fm, fs
                    box.cpp[at] = cx + ld(ms, u + 1, s + 1)
                    box.cpm[at] = -(cx + ld(ms, u + 1, s - 1))
                    box.inv[at] = inv
                    box.v[0][at] = v0
                    spread(box, 0, m + u, s, v0)
                    parts[u] = add(parts[u], clip(b * v0, span))
            return gather(box, m, acc, parts, inner)
        return run(loop, body, acc)

    def apply(box, k, loop, inner, accs):
        v, lx, ml, sl = box.v[k], box.sig[box.names[2]], box.sig[box.names[4]], box.sig[box.names[5]]

        def body(m, accs):
            ld = Cells(box, m)
            parts0, parts1 = [None] * loop[3], [None] * loop[3]
            for span in spans(box, 2 - k):
                s = span[0]
                for u in range(loop[3]):
                    at = (m + u, s)
                    val, hi, lo = ld(v, u, s), ld(v, u + 1, s), ld(v, u - 1, s)
                    up, down = ld(v, u, s + 1), ld(v, u, s - 1)
                    a1 = ld(box.fm, u, s) * hi + ld(box.fm, u - 1, s) * lo
                    a2 = ld(box.fs, u, s) * up + ld(box.fs, u, s - 1) * down
                    a3 = ld(box.cpp, u, s) * ld(v, u + 1, s + 1) + ld(box.cpp, u - 1, s - 1) * ld(v, u - 1, s - 1)
                    a4 = ld(box.cpm, u, s) * ld(v, u + 1, s - 1) + ld(box.cpm, u - 1, s + 1) * ld(v, u - 1, s + 1)
                    q = (ld(ml, u + 1, s) * hi - ld(ml, u - 1, s) * lo) + (
                        ld(sl, u, s + 1) * up - ld(sl, u, s - 1) * down)
                    a5 = ld(ml, u, s) * (ld(tin, u + 1, s) - ld(tin, u - 1, s))
                    a6 = ld(sl, u, s) * (ld(tin, u, s + 1) - ld(tin, u, s - 1))
                    c = ld(lx, u, s)
                    p = c * val
                    g = ((a1 + a2) + (a3 + a4)) + ((a5 + a6) + c * ld(zin, u, s)) + (left(p + q) + right(p - q))
                    parts0[u] = add(parts0[u], clip(val * g, span))
                    if k < 2:
                        nxt = g * ld(box.inv, u, s)
                        box.v[k + 1][at] = nxt
                        spread(box, k + 1, m + u, s, nxt)
                        parts1[u] = add(parts1[u], clip(nxt * g, span))
            acc0, acc1 = accs
            return gather(box, m, acc0, parts0, inner), gather(box, m, acc1, parts1, inner)

        tin, zin = box.t[k]
        return run(loop, body, accs)

    def extract(plane, trips):
        mine = [jnp.right_shift(lane, 4) == p for p in range(8)]

        def body(t, c):
            for src, dst in ((E.lab, k_lab), (E.b, k_b)):
                tiles = []
                for s in range(0, PY, 8):
                    tile = pltpu.roll(src[plane(t, 0), s], 8, 1)
                    for p in range(1, 8):
                        tile = jnp.where(mine[p], pltpu.roll(src[plane(t, p), s], (8 + 16 * p) % 128, 1), tile)
                    tiles.append(tile)
                tiles.append(jnp.zeros((128 - PY, 128), tile.dtype))
                turned = jnp.concatenate(tiles, axis=0).T
                for p in range(8):
                    x = plane(t, p)
                    dst[pl.ds(LAYERS * KX + x, 8, stride=KX), :] = turned[16 * p:16 * p + 8]
                    dst[pl.ds(4 * KX + x, 8, stride=KX), :] = turned[16 * p + 8:16 * p + 16]
            return c
        lax.fori_loop(0, trips, body, 0)

    own_rows = [W + 8 * i for i in range(Y // 8)]
    sigma(E, (W, 4, X // 4, 4), own_rows)
    arrive(lambda dx, dy: dx == 0)
    sigma(E, (W, 4, X // 4, 4), [0, PY - 8])
    extract(lambda t, p: W + 8 * t + p, X // 8)
    s0 = diagonal(E, (W + 1, 3, (X - 2) // 3, 3), None, zero)
    s12 = apply(E, 0, (W + 2, 4, (X - 4) // 4, 4), None, (zero, zero))

    arrive(lambda dx, dy: dx != 0)
    extract(lambda t, p: p + p // W * X, 1)
    sigma(E, (0, X + W, 2, 4), row_groups(0, PY))
    for field in (0, 1):
        for up in (0, 1):
            @pl.when(has[up])
            def _():
                phase2(up, field).start()

    s0 = diagonal(E, (1, X + 2, 2, 4), "ask", s0)
    s12 = apply(E, 0, (2, X, 2, 4), "ask", s12)
    s34 = apply(E, 1, (2, 4, (X + 4) // 4, 4), "ask", (zero, zero))
    s5, _ = apply(E, 2, (W, 4, X // 4, 4), None, (zero, zero))
    e_sums = [s0, *s12, *s34, s5]

    for field in (0, 1):
        for up in (0, 1):
            @pl.when(has[1 - up])
            def _():
                phase2(up, field).wait_recv()
    sigma(K, (0, 4, LAYERS // 2, 4), row_groups(0, PX))
    s0 = diagonal(K, (lambda t: 1 + 2 * t + (t // 5) * 2, 0, 10, 2), "ask", zero)
    s12 = apply(K, 0, (lambda t: 2 + 4 * t + (t // 2) * 4, 0, 4, 4), "ask", (zero, zero))
    s34 = apply(K, 1, (lambda t: 3 + 3 * t + (t // 2) * 6, 0, 4, 3), "ask", (zero, zero))
    s5, _ = apply(K, 2, (4, LAYERS, 2, 4), None, (zero, zero))
    k_sums = [s0, *s12, *s34, s5]

    edge = (lane < 4) | (lane >= 124)
    blocks = -(-X // 16)

    def complete():
        for k in range(3):
            for j in range(4):
                kint[pl.ds(j, X, stride=8), :] = k_arr[K.v[k].rows(LAYERS + 4 + j, W, X)]
                kint[pl.ds(4 + j, X, stride=8), :] = k_arr[K.v[k].rows(4 + j, W, X)]
            for q in range(blocks):
                kt[k, q] = kint[128 * q:128 * q + 128, :].T

        def body(m, c):
            for k in range(3):
                for s in range(W, W + Y, 8):
                    turned = pltpu.roll(kt[k, m // 16, pl.ds(s, 8), :], lax.rem(252 - 8 * lax.rem(m, 16), 128), 1)
                    E.v[k][m + W, s] = jnp.where(edge, turned, E.v[k][m + W, s])
            return c
        lax.fori_loop(0, X, body, 0, unroll=2)

    wide = lane[0:1]
    row = jnp.zeros((1, 128), jnp.float32)
    for k in range(6):
        from_k = jnp.where((wide >= W) & (wide < W + Y), jnp.sum(k_sums[k], axis=0, keepdims=True), 0.0)
        from_e = jnp.where((wide >= 4) & (wide < 124), jnp.sum(e_sums[k], axis=0, keepdims=True), 0.0)
        row = jnp.where(wide == k, jnp.sum(from_k + from_e, axis=1, keepdims=True), row)

    pl.semaphore_wait(greet.at[0], gxn - 1)
    slot = 0
    sent = []
    for stage, axes in enumerate(STAGES):
        ar[stage] = jnp.broadcast_to(row, (8, 128))
        copies = []
        first = slot
        for d in peers_of(axes):
            copy = pltpu.make_async_remote_copy(
                src_ref=ar.at[stage, pl.ds(0, 1), :], dst_ref=arslot.at[pl.ds(slot, 1), :], send_sem=sa.at[slot],
                recv_sem=ra.at[slot], device_id=peer(axes, d), device_id_type=MESH)
            copy.start()
            copies.append(copy)
            slot += 1
        if stage == 0:
            complete()
        for copy in copies:
            copy.wait_recv()
        row = row + jnp.sum(arslot[first:slot, :], axis=0, keepdims=True)
        sent += copies

    n = [jnp.broadcast_to(row[:, k:k + 1], (8, 128)) for k in range(6)]
    a = [n[k] - n[k + 1] for k in range(5)]
    safe = lambda num, den: jnp.where(den > 0, num / jnp.where(den > 0, den, 1.0), 0.0)
    l1, l2 = safe(a[1], a[0]), safe(a[2], a[0])
    d1 = a[2] - l1 * a[1]
    l21 = safe(a[3] - l1 * a[2], d1)
    d2 = a[4] - l2 * a[2] - l21 * (a[3] - l1 * a[2])
    y1 = n[1] - l1 * n[0]
    y2 = n[2] - l2 * n[0] - l21 * y1
    c2 = safe(y2, d2)
    c1 = safe(y1, d1) - l21 * c2
    c0 = safe(n[0], a[0]) - l1 * c1 - l2 * c2

    quarter = X // 4

    def put(t):
        part = pl.ds(t * quarter, quarter)
        return pltpu.make_async_copy(out.at[part], out_any.at[part], out_sem.at[t])

    def finish(t, c):
        for u in range(2):
            m = 2 * t + u
            for s in range(0, Y, 8):
                out[m, pl.ds(s, 8), :] = (c0 * E.v[0][m + W, s + W] + c1 * E.v[1][m + W, s + W]
                                          + c2 * E.v[2][m + W, s + W])
        return c

    def chunk(t, c):
        lax.fori_loop(t * (quarter // 2), (t + 1) * (quarter // 2), finish, 0)
        put(t).start()
        return c

    lax.fori_loop(0, 4, chunk, 0)

    for copy in sent:
        copy.wait_send()
    for field in (0, 1):
        for i, (dx, dy) in enumerate(DIRS):
            @pl.when(exists(dx, dy))
            def _():
                phase1(i, field).wait_send()
        for up in (0, 1):
            @pl.when(has[up])
            def _():
                phase2(up, field).wait_send()

    for t in range(4):
        put(t).wait()


def local(labels, conductivity, right_side, sizes):
    gxn, gyn, gzn = sizes
    X, Y, Z = labels.shape
    assert Z == 128 and Y % 8 == 0
    PX, PY = X + 2 * W, Y + 2 * W
    krows = 2 * LAYERS * (PX + 1)
    f32 = jnp.float32
    count = {"gx": gxn, "gy": gyn, "gz": gzn}
    slots = sum(math.prod(count[a] for a in axes) - 1 for axes in STAGES)
    dma = pltpu.SemaphoreType.DMA
    return pl.pallas_call(
        functools.partial(kernel, (gxn, gyn, gzn, X, Y)),
        out_shape=jax.ShapeDtypeStruct((X, Y, Z), f32),
        in_specs=[
            pl.BlockSpec(memory_space=pltpu.HBM),
            pl.BlockSpec(memory_space=pltpu.HBM),
            pl.BlockSpec(memory_space=pltpu.HBM),
        ],
        out_specs=pl.BlockSpec(memory_space=pl.ANY),
        scratch_shapes=[
            pltpu.VMEM((PX, PY, 128), jnp.int32),
            pltpu.VMEM((PX, PY, 128), f32),
            pltpu.VMEM((18 * (PX * PY + SKEW), 128), f32),
            pltpu.VMEM((krows, 128), jnp.int32),
            pltpu.VMEM((krows, 128), f32),
            pltpu.VMEM((18 * (krows + SKEW), 128), f32),
            pltpu.VMEM((-(-X // 16) * 128, 128), f32),
            pltpu.VMEM((3, -(-X // 16), 128, 128), f32),
            pltpu.VMEM((3, 8, 128), f32),
            pltpu.VMEM((slots, 128), f32),
            dma((3,)), dma((8, 2)), dma((8, 2)), dma((2, 2)), dma((2, 2)), dma((slots,)), dma((slots,)),
            pltpu.SemaphoreType.REGULAR((2,)), pltpu.VMEM((X, Y, Z), f32), dma((4,)),
            pltpu.SMEM((7, 8), f32),
        ],
        compiler_params=pltpu.CompilerParams(
            collective_id=0, has_side_effects=True, vmem_limit_bytes=62 * 1024 * 1024),
    )(conductivity, labels, right_side)


def solution(mesh):
    sizes = (mesh.shape["gx"], mesh.shape["gy"], mesh.shape["gz"])
    spec = P("gx", "gy", "gz")
    return jax.shard_map(
        functools.partial(local, sizes=sizes), mesh=mesh, in_specs=(spec, P(), spec), out_specs=spec, check_vma=False)
```
